32 devices in a mesh: groups: 2 (over x), expert: 16 (over z, y, core).
Axes of the slice: x: 2, y: 2, z: 4, core: 2. Of those that a mesh axis runs over, the one named last changes fastest.
Arguments:
- queries: bfloat16 [256, 4096], P(('groups', 'expert')), parts along dimension 0, may hold values from -150 to 150
- key_cache: bfloat16 [256, 64, 512], P(('groups', 'expert')), parts along dimension 0, may hold values from -7 to 7
- value_cache: bfloat16 [256, 64, 512], P(('groups', 'expert')), parts along dimension 0, may hold values from -6 to 6
- new_key: bfloat16 [256, 512], P(('groups', 'expert')), parts along dimension 0, may hold values from -6 to 6
- new_value: bfloat16 [256, 512], P(('groups', 'expert')), parts along dimension 0, may hold values from -6 to 6
- cache_lengths: int32 [256], P(('groups', 'expert')), parts along dimension 0, may hold values from 2 to 64, as said below
- hidden_in: bfloat16 [2048, 2048], P(('groups', 'expert')), parts along dimension 0, may hold values from -6 to 6
- norm_gain: bfloat16 [2048], replicated, may hold values from 0.5 to 1.5
- router_weight: bfloat16 [2048, 16], replicated, may hold values from -0.125 to 0.125
- expert_ids: int32 [2048, 8], P(('groups', 'expert')), parts along dimension 0, may hold values from 0 to 15, all different within a row; in each aligned block of 64 rows (0 to 63, 64 to 127, ...) at most 64 rows name the same one
- gate_train: bfloat16 [16, 2048, 768], P(None, 'expert'), may hold values from -0.125 to 0.125
- up_train: bfloat16 [16, 2048, 768], P(None, 'expert'), may hold values from -0.125 to 0.125
- down_train: bfloat16 [16, 768, 2048], P(None, 'expert'), may hold values from -0.21875 to 0.21875
Outputs:
- attended: bfloat16 [256, 4096], P(('groups', 'expert')), parts along dimension 0
- expert_mix: bfloat16 [2048, 2048], P(('groups', 'expert')), parts along dimension 0
The draws below stay inside these ranges and needn't reach their ends.
There are 2 independent parts, one for each index of `groups`. The reference program is written for one: setup_inputs(seed, part) draws one part's arguments, and reference() takes and returns one part's arrays. A program takes and returns all parts, laid end to end along the dimension named above; an argument that names none is the same for every part. Nothing has to cross between parts.
Inputs may be any that keep to these rules, and one draw needn't show every extreme that they name: `expert_ids`: each row names 8 different experts; within the rows of one device no expert is named more than 64 times. `cache_lengths`: the first sequence of each device's 8 has all 64 positions filled.
All inputs are finite; a program needn't handle non-finite values.
Results may differ from the reference program's by a relative error of at most 0.0074.
Values may be sent and summed in bfloat16 or wider, within the bound.
A program may use at most 128 MiB of HBM per device.

```python
import math
import jax
import jax.numpy as jnp
import numpy as np
from jax import lax

D = 2048
FF = 768
HEADS = 32
KV_HEADS = 4
HEAD_DIM = 128
TOP = 8
TOK_DEV = 64
ATT_DEV = 8
CTX = 64
EXPERTS = 16
TOKENS = 1024
SEQS = 128
CAP = 64
N_EXPERT = 16


def cache_base(key):
    return jnp.clip(jax.random.normal(jax.random.fold_in(key, 7), (SEQS, CTX, KV_HEADS * HEAD_DIM), jnp.float32), -6.0, 6.0)


def draw_key_cache(key, part):
    values = cache_base(key)
    return values.astype(jnp.bfloat16)


def draw_queries(key, part):
    values = jnp.clip(jax.random.normal(jax.random.fold_in(key, 9), (SEQS, HEADS * HEAD_DIM), jnp.float32), -6.0, 6.0)
    return values.astype(jnp.bfloat16)


def draw_cache_lengths(key, part):
    lengths = jax.random.randint(jax.random.fold_in(key, 12), (SEQS,), 2, CTX + 1, jnp.int32)
    return lengths.at[::ATT_DEV].set(CTX)


def levels(rng, shape, shards, low, top_value):
    loudness, own = 1.0, jax.random.fold_in(rng, 6)
    for dim, blocks in shards:
        heights = jnp.exp(jax.random.uniform(jax.random.fold_in(own, dim), (blocks,), jnp.float32, low / len(shards), top_value / len(shards)))
        loudness = loudness * jnp.repeat(heights, shape[dim] // blocks).reshape([-1 if axis == dim else 1 for axis in range(len(shape))])
    return loudness


def shared_out(key, own, number, rows, amount, top, bound, slope):
    order = jax.random.permutation(key, amount)
    heavy_load, common = shares(amount, rows * top, bound, slope, True), shares(amount, rows * top, bound, slope, False)
    places = jnp.arange(amount)

    def named(sizes, offset_by):
        used = int((sizes > 0).sum())
        fixed = max(1, used // 4)
        moved = fixed + (places - fixed + offset_by * (used - fixed)) % max(1, amount - fixed)
        return jnp.zeros((amount,), jnp.int32).at[order[jnp.where(places < fixed, places, moved)]].set(jnp.asarray(sizes, jnp.int32))

    sizes = jnp.where(number % 4 == 0, named(heavy_load, number // 4), named(common, number - number // 4 - 1))
    mixed = jax.random.permutation(jax.random.fold_in(own, 3), amount)
    giver, taker = mixed[0:amount // 2 * 2:2], mixed[1:amount // 2 * 2:2]
    margin = jnp.minimum(sizes[giver] - 1, bound - sizes[taker]) // 2
    margin = jnp.where((giver == order[0]) | (taker == order[0]) | (sizes[taker] == 0), 0, jnp.maximum(margin, 0))
    moved = jax.random.randint(jax.random.fold_in(own, 4), (amount // 2,), 0, 1 << 20) % (margin + 1)
    sizes = sizes.at[giver].add(-moved).at[taker].add(moved)
    labels = jnp.searchsorted(jnp.cumsum(sizes), jnp.arange(rows * top), side="right").astype(jnp.int32)
    listing = labels.reshape(top, rows).T
    listing = listing[jax.random.permutation(jax.random.fold_in(own, 1), rows)]
    offset_by = jax.random.randint(jax.random.fold_in(own, 2), (rows, 1), 0, top)
    return jnp.take_along_axis(listing, (jnp.arange(top)[None, :] + offset_by) % top, axis=1)


def shares(amount, total, reach, slope, full):
    loads = [(1 << 20) // math.isqrt(rank ** slope) + 1 for rank in range(1, amount + 1)]
    largest = reach if full else min(reach, max(-(-total // amount), total * loads[0] // sum(loads)))
    least = 1 if total - largest >= amount - 1 else 0
    holding, spare = [largest] + [least] * (amount - 1), total - largest - least * (amount - 1)
    while spare > 0:
        movable = [i for i in range(1, amount) if holding[i] < largest] or [i for i in range(1, amount) if holding[i] < reach]
        whole, left = sum([loads[i] for i in movable]), spare
        for i in movable:
            addition = min(reach - holding[i], max(1, left * loads[i] // whole), spare)
            holding[i] = holding[i] + addition
            spare = spare - addition
    return np.array(holding)


def centred(key, dims, width, limit, cuts=(), kind=jnp.bfloat16):
    result = width * jax.random.normal(key, dims, jnp.float32)
    if cuts:
        result = result * levels(key, dims, cuts, -0.22, 0.18)
    return jnp.clip(result, -limit, limit).astype(kind)


def setup_inputs(seed: int = 0, part: int = 0) -> dict:
    keys = jax.random.split(jax.random.key(seed), 14)
    part_keys = jax.random.split(jax.random.fold_in(keys[13], part), 14)
    queries = draw_queries(jax.random.fold_in(jax.random.fold_in(keys[13], part), 71), part)
    key_cache = draw_key_cache(jax.random.fold_in(jax.random.fold_in(keys[13], part), 71), part)
    value_cache = centred(part_keys[2], (SEQS, CTX, KV_HEADS * HEAD_DIM), 1.0, 6.0, ((0, 16),))
    new_key = centred(part_keys[3], (SEQS, KV_HEADS * HEAD_DIM), 1.0, 6.0, ((0, 16),))
    new_value = centred(part_keys[4], (SEQS, KV_HEADS * HEAD_DIM), 1.0, 6.0, ((0, 16),))
    cache_lengths = draw_cache_lengths(jax.random.fold_in(jax.random.fold_in(keys[13], part), 71), part)
    hidden_in = centred(part_keys[6], (TOKENS, D), 1.0, 6.0, ((0, 16),))
    norm_gain = jnp.clip(1.0 + 0.1 * jax.random.normal(keys[7], (D,), jnp.float32), 0.5, 1.5).astype(jnp.bfloat16)
    router_weight = centred(keys[8], (D, EXPERTS), D ** -0.5, 0.125)
    expert_ids_keys = jax.random.split(jax.random.fold_in(part_keys[9], 1), TOKENS // TOK_DEV)
    expert_ids_turns = jax.random.permutation(jax.random.fold_in(part_keys[9], 3), TOKENS // TOK_DEV)
    expert_ids = jax.vmap(lambda own, number: shared_out(jax.random.fold_in(part_keys[9], 2), own, number, TOK_DEV, EXPERTS, TOP, CAP, 1))(expert_ids_keys, expert_ids_turns).reshape((TOKENS, TOP))
    gate_train = centred(keys[10], (EXPERTS, D, FF), D ** -0.5, 0.125, ((1, 16),))
    up_train = centred(keys[11], (EXPERTS, D, FF), D ** -0.5, 0.125, ((1, 16),))
    down_train = centred(keys[12], (EXPERTS, FF, D), FF ** -0.5, 0.21875, ((1, 16),))
    return dict(queries=queries, key_cache=key_cache, value_cache=value_cache, new_key=new_key, new_value=new_value, cache_lengths=cache_lengths, hidden_in=hidden_in, norm_gain=norm_gain, router_weight=router_weight, expert_ids=expert_ids, gate_train=gate_train, up_train=up_train, down_train=down_train)


EPSILON = 1e-06

def rms_normed(hidden_in, norm_gain):
    values = hidden_in.astype(jnp.float32)
    mean_square = lax.optimization_barrier(jnp.mean(values * values, axis=-1, keepdims=True))
    return (values * lax.rsqrt(mean_square + EPSILON) * norm_gain.astype(jnp.float32)).astype(jnp.bfloat16)

def attend(queries, key_cache, value_cache, new_key, new_value, cache_lengths):
    seq_count = queries.shape[0]
    group_size = HEADS // KV_HEADS
    query_blocks = queries.astype(jnp.float32).reshape(seq_count, KV_HEADS, group_size, HEAD_DIM)
    cached_keys = key_cache.astype(jnp.float32).reshape(seq_count, CTX, KV_HEADS, HEAD_DIM)
    cached_values = value_cache.astype(jnp.float32).reshape(seq_count, CTX, KV_HEADS, HEAD_DIM)
    fresh_keys = new_key.astype(jnp.float32).reshape(seq_count, KV_HEADS, HEAD_DIM)
    fresh_values = new_value.astype(jnp.float32).reshape(seq_count, KV_HEADS, HEAD_DIM)
    score_scale = 1.0 / math.sqrt(HEAD_DIM)
    scores = jnp.einsum('sgrd,scgd->sgrc', query_blocks, cached_keys) * score_scale
    own_score = jnp.einsum('sgrd,sgd->sgr', query_blocks, fresh_keys) * score_scale
    positions = jnp.arange(CTX, dtype=jnp.int32)
    visible = positions[None, :] < cache_lengths.astype(jnp.int32)[:, None]
    scores = jnp.where(visible[:, None, None, :], scores, -1e+30)
    largest = jnp.maximum(lax.optimization_barrier(jnp.max(scores, axis=-1)), own_score)
    cached_exp = jnp.exp(scores - largest[..., None])
    own_exp = jnp.exp(own_score - largest)
    prob_total = lax.optimization_barrier(jnp.sum(cached_exp, axis=-1)) + own_exp
    cached_prob = lax.optimization_barrier((cached_exp / prob_total[..., None]).astype(jnp.bfloat16)).astype(jnp.float32)
    own_prob = lax.optimization_barrier((own_exp / prob_total).astype(jnp.bfloat16)).astype(jnp.float32)
    context = jnp.einsum('sgrc,scgd->sgrd', cached_prob, cached_values)
    context = context + own_prob[..., None] * fresh_values[:, :, None, :]
    return context.reshape(seq_count, HEADS * HEAD_DIM).astype(jnp.bfloat16)

def expert_block(operands):
    token_rows, gate_weight, up_weight, down_weight = operands
    gate_proj = jnp.dot(token_rows, gate_weight, preferred_element_type=jnp.float32)
    up_proj = jnp.dot(token_rows, up_weight, preferred_element_type=jnp.float32)
    hidden_units = (jax.nn.silu(gate_proj) * up_proj).astype(jnp.bfloat16)
    return jnp.dot(hidden_units, down_weight, preferred_element_type=jnp.float32).astype(jnp.bfloat16)

def mix_experts(hidden_in, norm_gain, router_weight, expert_ids, gate_train, up_train, down_train):
    normed = rms_normed(hidden_in, norm_gain)
    logits = jnp.dot(normed, router_weight, preferred_element_type=jnp.float32)
    expert_range = jnp.arange(EXPERTS, dtype=jnp.int32)
    picked = expert_ids.astype(jnp.int32)[:, :, None] == expert_range[None, None, :]
    chosen = lax.optimization_barrier(jnp.sum(jnp.where(picked, logits[:, None, :], 0.0), axis=-1))
    mixing = jax.nn.softmax(chosen, axis=-1)
    onehot_int = picked.astype(jnp.int32).reshape(N_EXPERT, TOK_DEV * TOP, EXPERTS)
    rank_values = lax.optimization_barrier(jnp.sum((jnp.cumsum(onehot_int, axis=1).astype(jnp.int32) - 1) * onehot_int, axis=-1)).astype(jnp.int32)
    sources = jnp.arange(N_EXPERT, dtype=jnp.int32)[:, None]
    slot_index = (sources * CAP + rank_values).reshape(-1).astype(jnp.int32)
    flat_ids = expert_ids.reshape(-1).astype(jnp.int32)
    repeated = jnp.repeat(normed, TOP, axis=0)
    buffers = jnp.zeros((EXPERTS, N_EXPERT * CAP, D), jnp.bfloat16).at[flat_ids, slot_index].set(repeated)
    outputs = lax.map(expert_block, (buffers, gate_train, up_train, down_train))
    returned = outputs[flat_ids, slot_index].astype(jnp.float32).reshape(TOKENS, TOP, D)
    return lax.optimization_barrier(jnp.sum(mixing[:, :, None] * returned, axis=1)).astype(jnp.bfloat16)

def reference(queries, key_cache, value_cache, new_key, new_value, cache_lengths, hidden_in, norm_gain, router_weight, expert_ids, gate_train, up_train, down_train):
    attended = attend(queries, key_cache, value_cache, new_key, new_value, cache_lengths)
    expert_mix = mix_experts(hidden_in, norm_gain, router_weight, expert_ids, gate_train, up_train, down_train)
    return (attended, expert_mix)
```

```python
import math

import jax
import jax.numpy as jnp
from jax import lax
from jax.sharding import PartitionSpec as P

HEADS = 32
KV_HEADS = 4
HEAD_DIM = 128
CTX = 64


EPSILON = 1e-06


def rms_normed(hidden_in, norm_gain):
    values = hidden_in.astype(jnp.float32)
    mean_square = jnp.mean(values * values, axis=-1, keepdims=True)
    return (values * lax.rsqrt(mean_square + EPSILON) * norm_gain.astype(jnp.float32)).astype(
        jnp.bfloat16
    )


def attend(queries, key_cache, value_cache, new_key, new_value, cache_lengths):
    seq_count = queries.shape[0]
    group_size = HEADS // KV_HEADS
    query_blocks = queries.reshape(seq_count, KV_HEADS, group_size, HEAD_DIM)
    cached_keys = key_cache.reshape(seq_count, CTX, KV_HEADS, HEAD_DIM)
    cached_values = value_cache.reshape(seq_count, CTX, KV_HEADS, HEAD_DIM)
    fresh_keys = new_key.reshape(seq_count, KV_HEADS, HEAD_DIM)
    fresh_values = new_value.astype(jnp.float32).reshape(seq_count, KV_HEADS, HEAD_DIM)
    score_scale = 1.0 / math.sqrt(HEAD_DIM)
    scores = (
        jnp.einsum("sgrd,scgd->sgrc", query_blocks, cached_keys, preferred_element_type=jnp.float32)
        * score_scale
    )
    own_score = (
        jnp.einsum("sgrd,sgd->sgr", query_blocks, fresh_keys, preferred_element_type=jnp.float32)
        * score_scale
    )
    positions = jnp.arange(CTX, dtype=jnp.int32)
    visible = positions[None, :] < cache_lengths[:, None]
    scores = jnp.where(visible[:, None, None, :], scores, -1e30)
    largest = jnp.maximum(jnp.max(scores, axis=-1), own_score)
    cached_exp = jnp.exp(scores - largest[..., None])
    own_exp = jnp.exp(own_score - largest)
    prob_total = jnp.sum(cached_exp, axis=-1) + own_exp
    cached_prob = (cached_exp / prob_total[..., None]).astype(jnp.bfloat16)
    own_prob = (own_exp / prob_total).astype(jnp.bfloat16).astype(jnp.float32)
    context = jnp.einsum(
        "sgrc,scgd->sgrd", cached_prob, cached_values, preferred_element_type=jnp.float32
    )
    context = context + own_prob[..., None] * fresh_values[:, :, None, :]
    return context.reshape(seq_count, HEADS * HEAD_DIM).astype(jnp.bfloat16)


def dense_mixing(normed, router_weight, expert_ids):
    logits = jnp.dot(normed, router_weight, preferred_element_type=jnp.float32)
    expert_range = jnp.arange(router_weight.shape[1], dtype=jnp.int32)
    picked = jnp.any(expert_ids[:, :, None] == expert_range[None, None, :], axis=1)
    masked = jnp.where(picked, logits, -jnp.inf)
    raised = jnp.exp(masked - jnp.max(masked, axis=-1, keepdims=True))
    return raised / jnp.sum(raised, axis=-1, keepdims=True)


def local(
    queries,
    key_cache,
    value_cache,
    new_key,
    new_value,
    cache_lengths,
    hidden_in,
    norm_gain,
    router_weight,
    expert_ids,
    gate_train,
    up_train,
    down_train,
):
    width = hidden_in.shape[1]
    expert_count = router_weight.shape[1]
    normed = rms_normed(hidden_in, norm_gain)
    mixing = dense_mixing(normed, router_weight, expert_ids)
    mixing_high = mixing.astype(jnp.bfloat16)
    mixing_low = (mixing - mixing_high.astype(jnp.float32)).astype(jnp.bfloat16)
    spare = -2 * expert_count % 128
    row_block = jnp.concatenate(
        [normed, mixing_high, mixing_low, jnp.zeros((normed.shape[0], spare), jnp.bfloat16)], axis=1
    )
    all_rows = lax.all_gather(row_block, "expert", axis=0, tiled=True)
    gate_moved = lax.all_to_all(gate_train, "expert", split_axis=0, concat_axis=1, tiled=True)[0]
    up_moved = lax.all_to_all(up_train, "expert", split_axis=0, concat_axis=1, tiled=True)[0]
    attended = attend(queries, key_cache, value_cache, new_key, new_value, cache_lengths)
    own_index = lax.axis_index("expert")
    tokens = all_rows[:, :width]
    mix_parts = all_rows[:, width : width + 2 * expert_count].astype(jnp.float32)
    own_column = jnp.arange(2 * expert_count) % expert_count == own_index
    own_mix = jnp.sum(jnp.where(own_column[None, :], mix_parts, 0.0), axis=1)
    contract = (((0,), (1,)), ((), ()))
    gate_proj = lax.dot_general(gate_moved, tokens, contract, preferred_element_type=jnp.float32)
    up_proj = lax.dot_general(up_moved, tokens, contract, preferred_element_type=jnp.float32)
    hidden_units = (jax.nn.silu(gate_proj) * up_proj * own_mix[None, :]).astype(jnp.bfloat16)
    hidden_all = lax.all_to_all(hidden_units, "expert", split_axis=0, concat_axis=0, tiled=True)
    partial_out = lax.dot_general(
        hidden_all,
        down_train.reshape(-1, width),
        (((0,), (0,)), ((), ())),
        preferred_element_type=jnp.float32,
    ).astype(jnp.bfloat16)
    mixed_out = lax.psum_scatter(partial_out, "expert", scatter_dimension=0, tiled=True)
    return (attended, mixed_out)


def solution(mesh):
    placed = (
        P(("groups", "expert"), None),
        P(("groups", "expert"), None, None),
        P(("groups", "expert"), None, None),
        P(("groups", "expert"), None),
        P(("groups", "expert"), None),
        P(("groups", "expert")),
        P(("groups", "expert"), None),
        P(),
        P(),
        P(("groups", "expert"), None),
        P(None, "expert", None),
        P(None, "expert", None),
        P(None, "expert", None),
    )
    return jax.shard_map(
        local,
        mesh=mesh,
        in_specs=placed,
        out_specs=(P(("groups", "expert"), None), P(("groups", "expert"), None)),
        check_vma=False,
    )
```

```python
import functools
import math

import jax
import jax.numpy as jnp
from jax import lax
from jax.experimental import pallas as pl
from jax.experimental.pallas import tpu as pltpu
from jax.sharding import PartitionSpec as P

HEADS = 32
KV_HEADS = 4
HEAD_DIM = 128
CTX = 64


EPSILON = 1e-06


def rms_normed(hidden_in, norm_gain):
    values = hidden_in.astype(jnp.float32)
    mean_square = jnp.mean(values * values, axis=-1, keepdims=True)
    return (values * lax.rsqrt(mean_square + EPSILON) * norm_gain.astype(jnp.float32)).astype(
        jnp.bfloat16
    )


def attend(queries, key_cache, value_cache, new_key, new_value, cache_lengths):
    seq_count = queries.shape[0]
    group_size = HEADS // KV_HEADS
    query_blocks = queries.reshape(seq_count, KV_HEADS, group_size, HEAD_DIM)
    cached_keys = key_cache.reshape(seq_count, CTX, KV_HEADS, HEAD_DIM)
    cached_values = value_cache.reshape(seq_count, CTX, KV_HEADS, HEAD_DIM)
    fresh_keys = new_key.reshape(seq_count, KV_HEADS, HEAD_DIM)
    fresh_values = new_value.astype(jnp.float32).reshape(seq_count, KV_HEADS, HEAD_DIM)
    score_scale = 1.0 / math.sqrt(HEAD_DIM)
    scores = (
        jnp.einsum("sgrd,scgd->sgrc", query_blocks, cached_keys, preferred_element_type=jnp.float32)
        * score_scale
    )
    own_score = (
        jnp.einsum("sgrd,sgd->sgr", query_blocks, fresh_keys, preferred_element_type=jnp.float32)
        * score_scale
    )
    positions = jnp.arange(CTX, dtype=jnp.int32)
    visible = positions[None, :] < cache_lengths[:, None]
    scores = jnp.where(visible[:, None, None, :], scores, -1e30)
    largest = jnp.maximum(jnp.max(scores, axis=-1), own_score)
    cached_exp = jnp.exp(scores - largest[..., None])
    own_exp = jnp.exp(own_score - largest)
    prob_total = jnp.sum(cached_exp, axis=-1) + own_exp
    cached_prob = (cached_exp / prob_total[..., None]).astype(jnp.bfloat16)
    own_prob = (own_exp / prob_total).astype(jnp.bfloat16).astype(jnp.float32)
    context = jnp.einsum(
        "sgrc,scgd->sgrd", cached_prob, cached_values, preferred_element_type=jnp.float32
    )
    context = context + own_prob[..., None] * fresh_values[:, :, None, :]
    return context.reshape(seq_count, HEADS * HEAD_DIM).astype(jnp.bfloat16)


def dense_mixing(normed, router_weight, expert_ids):
    logits = jnp.dot(normed, router_weight, preferred_element_type=jnp.float32)
    expert_range = jnp.arange(router_weight.shape[1], dtype=jnp.int32)
    picked = jnp.any(expert_ids[:, :, None] == expert_range[None, None, :], axis=1)
    masked = jnp.where(picked, logits, -jnp.inf)
    raised = jnp.exp(masked - jnp.max(masked, axis=-1, keepdims=True))
    return raised / jnp.sum(raised, axis=-1, keepdims=True)


MESH = pl.DeviceIdType.MESH
AHEAD = 8


def greet(targets):
    barrier = pltpu.get_barrier_semaphore()

    expected = 0
    for condition, target in targets:
        signal = functools.partial(
            pl.semaphore_signal, barrier, inc=1, device_id=target, device_id_type=MESH
        )
        if condition is None:
            signal()
            expected = expected + 1
        else:
            pl.when(condition)(signal)
            expected = expected + condition.astype(jnp.int32)
    pl.semaphore_wait(barrier, expected)


def move_kernel(
    groups, count,
    gate_ref, up_ref, down_ref, rows_ref,
    gate_out, up_out, down_out, rows_out,
    send_w, recv_w, send_x, recv_x, local_sem, send_rows, recv_rows,
):
    me = lax.axis_index("expert")
    group = lax.axis_index("groups")
    parts = max(1, groups // 2)
    part_rows = gate_ref.shape[1] // parts
    part_columns = down_ref.shape[2] // groups
    line = count // 4
    layer = me // 4

    others = [(None, (group, me ^ r)) for r in range(1, count)]
    others += [(None, (lax.rem(group + h, groups), me)) for h in range(1, groups)]
    greet(others)

    def remote(src, dst, send, recv, target):
        return pltpu.make_async_remote_copy(
            src_ref=src, dst_ref=dst, send_sem=send, recv_sem=recv, device_id=target, device_id_type=MESH
        )

    def rows_of(owner):
        return pl.ds(pl.multiple_of((owner // 2) * part_rows, part_rows), part_rows)

    def columns_of(owner):
        return pl.ds(pl.multiple_of(owner * part_columns, part_columns), part_columns)

    def row_copy(kind, block, target, own=False):
        source = rows_ref if own else rows_out.at[block]
        return remote(
            source, rows_out.at[block], send_rows.at[kind, block], recv_rows.at[block], (group, target)
        )

    def row_wait(block):
        row_copy(0, block, me ^ 1).wait_recv()

    own_rows = pltpu.make_async_copy(rows_ref, rows_out.at[me], local_sem.at[3])
    own_rows.start()
    has_up, has_down = me + 4 < count, me >= 4

    @pl.when(has_up)
    def _():
        row_copy(0, me, me + 4, True).start()

    @pl.when(has_down)
    def _():
        row_copy(1, me, me - 4, True).start()

    row_copy(2, me, me ^ 2, True).start()
    row_copy(3, me, me ^ 1, True).start()

    def line_step(step):
        below, above = me - 4 * (step + 1), me + 4 * (step + 1)

        @pl.when(below >= 0)
        def _():
            row_wait(below)

            @pl.when(has_up)
            def _():
                row_copy(0, below, me + 4).start()

            row_copy(2, below, me ^ 2).start()
            row_copy(3, below, me ^ 1).start()

        @pl.when(above < count)
        def _():
            row_wait(above)

            @pl.when(has_down)
            def _():
                row_copy(1, above, me - 4).start()

            row_copy(2, above, me ^ 2).start()
            row_copy(3, above, me ^ 1).start()

    def side_step(index):
        block = lax.rem(me, 4) ^ 2
        block = block + 4 * index
        row_wait(block)
        row_copy(3, block, me ^ 1).start()

    def across(kind, r, refs_in, refs_out, which):
        target = me ^ r
        if kind == 0:
            return remote(
                refs_in[which].at[target, rows_of(group)], refs_out[which].at[me, rows_of(group)],
                send_w.at[0, r], recv_w.at[0, r], (group, target),
            )
        return remote(
            down_ref.at[target, :, columns_of(group)], down_out.at[me, :, columns_of(group)],
            send_w.at[1, r], recv_w.at[1, r], (group, target),
        )

    ins, outs = (gate_ref, up_ref), (gate_out, up_out)

    def by_matrix(act):
        pl.when(lax.rem(group, 2) == 0)(functools.partial(act, 0))
        pl.when(lax.rem(group, 2) == 1)(functools.partial(act, 1))

    def start_weight(kind, r):
        if kind == 0:
            by_matrix(lambda which: across(0, r, ins, outs, which).start())
        else:
            across(1, r, ins, outs, 0).start()

    def onward(kind, r, h, which):
        held = me ^ r
        place = outs[which].at[held, rows_of(group)] if kind == 0 else down_out.at[held, :, columns_of(group)]
        return remote(
            place, place, send_x.at[kind, r, h - 1], recv_x.at[kind, r, h - 1],
            (lax.rem(group + h, groups), me),
        )

    def pass_on(kind, r):
        across(kind, r, ins, outs, 0).wait_recv()
        for h in range(1, groups):
            if kind == 0:
                by_matrix(lambda which: onward(0, r, h, which).start())
            else:
                onward(1, r, h, 0).start()

    own_copies = [
        pltpu.make_async_copy(a.at[me], b.at[me], local_sem.at[i])
        for i, (a, b) in enumerate(((gate_ref, gate_out), (up_ref, up_out), (down_ref, down_out)))
    ]
    half = count // 2
    order = [r for i in range(half) for r in ((half + i, i) if i else (half,))]
    items = [(kind, r) for kind in range(2) for r in order]
    side_at = 3 + 2 * (line - 1) + 2
    for i, item in enumerate(items):
        start_weight(*item)
        if i >= 3 and (i - 3) % 2 == 0 and (i - 3) // 2 < line - 1:
            line_step((i - 3) // 2)
        if i == side_at:
            for index in range(line):
                side_step(index)
        if i == AHEAD:
            for copy in own_copies:
                copy.start()
        if i >= AHEAD:
            pass_on(*items[i - AHEAD])
    for item in items[len(items) - AHEAD :]:
        pass_on(*item)

    for index in range(line):
        for y in range(2):
            row_wait(4 * index + 2 * y + (lax.rem(me, 2) ^ 1))
    own_rows.wait()
    for copy in own_copies:
        copy.wait()
    for kind, r in items:
        across(kind, r, ins, outs, 0).wait_send()
        for h in range(1, groups):
            onward(kind, r, h, 0).wait()
    for index in range(line):
        block = lax.rem(me, 4) + 4 * index

        @pl.when(jnp.logical_and(has_up, index <= layer))
        def _():
            row_copy(0, block, me ^ 1).wait_send()

        @pl.when(jnp.logical_and(has_down, index >= layer))
        def _():
            row_copy(1, block, me ^ 1).wait_send()

        row_copy(2, block, me ^ 1).wait_send()
        row_copy(3, block, me ^ 1).wait_send()
        row_copy(3, block ^ 2, me ^ 1).wait_send()


def move(groups, gate_train, up_train, down_train, row_block):
    count = gate_train.shape[0]
    anywhere = pl.BlockSpec(memory_space=pl.ANY)
    DMA = pltpu.SemaphoreType.DMA
    return pl.pallas_call(
        functools.partial(move_kernel, groups, count),
        out_shape=[
            jax.ShapeDtypeStruct(gate_train.shape, gate_train.dtype),
            jax.ShapeDtypeStruct(up_train.shape, up_train.dtype),
            jax.ShapeDtypeStruct(down_train.shape, down_train.dtype),
            jax.ShapeDtypeStruct((count,) + row_block.shape, row_block.dtype),
        ],
        in_specs=[anywhere, anywhere, anywhere, pl.BlockSpec(memory_space=pltpu.VMEM)],
        out_specs=[anywhere] * 4,
        scratch_shapes=[
            DMA((2, count)), DMA((2, count)),
            DMA((2, count, max(1, groups - 1))), DMA((2, count, max(1, groups - 1))),
            DMA((4,)), DMA((4, count)), DMA((count,)),
        ],
        compiler_params=pltpu.CompilerParams(collective_id=0, has_side_effects=True),
    )(gate_train, up_train, down_train, row_block)


def sum_kernel(
    count, part_ref, out_ref, core_in, side_in, up_in, down_in, side_out, up_out, down_out,
    core_send, core_recv, side_send, side_recv, up_send, up_recv, down_send, down_recv,
):
    me = lax.axis_index("expert")
    group = lax.axis_index("groups")
    line, layer = count // 4, me // 4
    place = lax.rem(me, 4)
    side, core = place // 2, lax.rem(place, 2)
    has_up, has_down = me + 4 < count, me >= 4
    greet([
        (None, (group, me ^ 1)), (None, (group, me ^ 2)),
        (has_up, (group, me + 4)), (has_down, (group, me - 4)),
    ])
    chunk = 16
    row_count = part_ref.shape[1]

    def remote(src, dst, send, recv, target):
        return pltpu.make_async_remote_copy(
            src_ref=src, dst_ref=dst, send_sem=send, recv_sem=recv, device_id=(group, target), device_id_type=MESH
        )

    def add(target, *sources):
        @pl.loop(0, row_count // chunk)
        def _(step):
            rows = pl.ds(pl.multiple_of(step * chunk, chunk), chunk)
            total = sources[0][rows, :].astype(jnp.float32)
            for source in sources[1:]:
                total = total + source[rows, :].astype(jnp.float32)
            target[rows, :] = total.astype(target.dtype)

    def core_copy(at, y):
        slot = at * 2 + y
        return remote(
            part_ref.at[at * 4 + y * 2 + (core ^ 1)], core_in.at[slot], core_send.at[slot], core_recv.at[slot], me ^ 1
        )

    def side_copy(at):
        return remote(side_out.at[at], side_in.at[at], side_send.at[at], side_recv.at[at], me ^ 2)

    def up_copy(at):
        return remote(up_out.at[at], up_in.at[at], up_send.at[at], up_recv.at[at], me + 4)

    def down_copy(at):
        return remote(down_out.at[at], down_in.at[at], down_send.at[at], down_recv.at[at], me - 4)

    def in_order(act):
        for d in range(line - 1, 0, -1):
            pl.when(layer + d < line)(functools.partial(act, layer + d, 1))
            pl.when(layer - d >= 0)(functools.partial(act, layer - d, -1))
        act(layer, 0)

    in_order(lambda at, way: core_copy(at, side ^ 1).start())
    in_order(lambda at, way: core_copy(at, side).start())

    def to_side(at, way):
        core_copy(at, side ^ 1).wait_recv()
        add(side_out.at[at], part_ref.at[at * 4 + (side ^ 1) * 2 + core], core_in.at[at * 2 + (side ^ 1)])
        side_copy(at).start()

    in_order(to_side)

    def along(at, way):
        core_copy(at, side).wait_recv()
        side_copy(at).wait_recv()
        mine = (part_ref.at[at * 4 + place], core_in.at[at * 2 + side], side_in.at[at])
        if way == 1:
            @pl.when(has_down)
            def _():
                up_copy(at).wait_recv()
                add(up_out.at[at], *mine, up_in.at[at])

            @pl.when(jnp.logical_not(has_down))
            def _():
                add(up_out.at[at], *mine)

            up_copy(at).start()
        elif way == -1:
            @pl.when(has_up)
            def _():
                down_copy(at).wait_recv()
                add(down_out.at[at], *mine, down_in.at[at])

            @pl.when(jnp.logical_not(has_up))
            def _():
                add(down_out.at[at], *mine)

            down_copy(at).start()
        else:
            @pl.when(has_down)
            def _():
                up_copy(at).wait_recv()

            @pl.when(has_up)
            def _():
                down_copy(at).wait_recv()

            both = jnp.logical_and(has_down, has_up)

            @pl.when(both)
            def _():
                add(out_ref, *mine, up_in.at[at], down_in.at[at])

            @pl.when(jnp.logical_and(has_down, jnp.logical_not(has_up)))
            def _():
                add(out_ref, *mine, up_in.at[at])

            @pl.when(jnp.logical_and(has_up, jnp.logical_not(has_down)))
            def _():
                add(out_ref, *mine, down_in.at[at])

            @pl.when(jnp.logical_not(jnp.logical_or(has_up, has_down)))
            def _():
                add(out_ref, *mine)

    in_order(along)

    def finish(at, way):
        core_copy(at, side ^ 1).wait_send()
        core_copy(at, side).wait_send()
        side_copy(at).wait_send()
        if way == 1:
            up_copy(at).wait_send()
        if way == -1:
            down_copy(at).wait_send()

    in_order(finish)


def summed(partial_out, count):
    rows, width = partial_out.shape[0] // count, partial_out.shape[1]
    line = count // 4
    DMA = pltpu.SemaphoreType.DMA
    block = lambda amount: pltpu.VMEM((amount, rows, width), jnp.bfloat16)
    return pl.pallas_call(
        functools.partial(sum_kernel, count),
        out_shape=jax.ShapeDtypeStruct((rows, width), jnp.bfloat16),
        in_specs=[pl.BlockSpec(memory_space=pltpu.VMEM)],
        out_specs=pl.BlockSpec(memory_space=pltpu.VMEM),
        scratch_shapes=[block(count // 2)] + [block(line)] * 6
        + [DMA((count // 2,)), DMA((count // 2,))] + [DMA((line,))] * 6,
        compiler_params=pltpu.CompilerParams(collective_id=1, has_side_effects=True, vmem_limit_bytes=60 * 2**20),
    )(partial_out.reshape(count, rows, width))


def local(
    queries,
    key_cache,
    value_cache,
    new_key,
    new_value,
    cache_lengths,
    hidden_in,
    norm_gain,
    router_weight,
    expert_ids,
    gate_train,
    up_train,
    down_train,
):
    width = hidden_in.shape[1]
    expert_count = router_weight.shape[1]
    normed = rms_normed(hidden_in, norm_gain)
    mixing = dense_mixing(normed, router_weight, expert_ids)
    mixing_high = mixing.astype(jnp.bfloat16)
    mixing_low = (mixing - mixing_high.astype(jnp.float32)).astype(jnp.bfloat16)
    spare = -2 * expert_count % 128
    row_block = jnp.concatenate(
        [normed, mixing_high, mixing_low, jnp.zeros((normed.shape[0], spare), jnp.bfloat16)], axis=1
    )
    gate_moved, up_moved, down_moved, all_rows = move(
        lax.axis_size("groups"), gate_train, up_train, down_train, row_block
    )
    all_rows = all_rows.reshape(-1, all_rows.shape[-1])
    gate_moved = gate_moved.reshape(-1, gate_moved.shape[-1])
    up_moved = up_moved.reshape(-1, up_moved.shape[-1])
    down_moved = down_moved.reshape(-1, width)
    attended = attend(queries, key_cache, value_cache, new_key, new_value, cache_lengths)
    own_index = lax.axis_index("expert")
    tokens = all_rows[:, :width]
    mix_parts = all_rows[:, width : width + 2 * expert_count].astype(jnp.float32)
    own_column = jnp.arange(2 * expert_count) % expert_count == own_index
    own_mix = jnp.sum(jnp.where(own_column[None, :], mix_parts, 0.0), axis=1)
    gate_proj = jnp.dot(tokens, gate_moved, preferred_element_type=jnp.float32)
    up_proj = jnp.dot(tokens, up_moved, preferred_element_type=jnp.float32)
    hidden_units = (jax.nn.silu(gate_proj) * up_proj * own_mix[:, None]).astype(jnp.bfloat16)
    partial_out = jnp.dot(hidden_units, down_moved, preferred_element_type=jnp.float32).astype(jnp.bfloat16)
    mixed_out = summed(partial_out, expert_count)
    return (attended, mixed_out)


def solution(mesh):
    placed = (
        P(("groups", "expert"), None),
        P(("groups", "expert"), None, None),
        P(("groups", "expert"), None, None),
        P(("groups", "expert"), None),
        P(("groups", "expert"), None),
        P(("groups", "expert")),
        P(("groups", "expert"), None),
        P(),
        P(),
        P(("groups", "expert"), None),
        P(None, "expert", None),
        P(None, "expert", None),
        P(None, "expert", None),
    )
    return jax.shard_map(
        local,
        mesh=mesh,
        in_specs=placed,
        out_specs=(P(("groups", "expert"), None), P(("groups", "expert"), None)),
        check_vma=False,
    )
```

```python
import functools
import math

import jax
import jax.numpy as jnp
from jax import lax
from jax.experimental import pallas as pl
from jax.experimental.pallas import tpu as pltpu
from jax.sharding import PartitionSpec as P

HEADS = 32
KV_HEADS = 4
HEAD_DIM = 128
CTX = 64


EPSILON = 1e-06


def rms_normed(hidden_in, norm_gain):
    values = hidden_in.astype(jnp.float32)
    mean_square = jnp.mean(values * values, axis=-1, keepdims=True)
    return (values * lax.rsqrt(mean_square + EPSILON) * norm_gain.astype(jnp.float32)).astype(
        jnp.bfloat16
    )


def attend(queries, key_cache, value_cache, new_key, new_value, cache_lengths):
    seq_count = queries.shape[0]
    group_size = HEADS // KV_HEADS
    query_blocks = queries.reshape(seq_count, KV_HEADS, group_size, HEAD_DIM)
    cached_keys = key_cache.reshape(seq_count, CTX, KV_HEADS, HEAD_DIM)
    cached_values = value_cache.reshape(seq_count, CTX, KV_HEADS, HEAD_DIM)
    fresh_keys = new_key.reshape(seq_count, KV_HEADS, HEAD_DIM)
    fresh_values = new_value.astype(jnp.float32).reshape(seq_count, KV_HEADS, HEAD_DIM)
    score_scale = 1.0 / math.sqrt(HEAD_DIM)
    scores = (
        jnp.einsum("sgrd,scgd->sgrc", query_blocks, cached_keys, preferred_element_type=jnp.float32)
        * score_scale
    )
    own_score = (
        jnp.einsum("sgrd,sgd->sgr", query_blocks, fresh_keys, preferred_element_type=jnp.float32)
        * score_scale
    )
    positions = jnp.arange(CTX, dtype=jnp.int32)
    visible = positions[None, :] < cache_lengths[:, None]
    scores = jnp.where(visible[:, None, None, :], scores, -1e30)
    largest = jnp.maximum(jnp.max(scores, axis=-1), own_score)
    cached_exp = jnp.exp(scores - largest[..., None])
    own_exp = jnp.exp(own_score - largest)
    prob_total = jnp.sum(cached_exp, axis=-1) + own_exp
    cached_prob = (cached_exp / prob_total[..., None]).astype(jnp.bfloat16)
    own_prob = (own_exp / prob_total).astype(jnp.bfloat16).astype(jnp.float32)
    context = jnp.einsum(
        "sgrc,scgd->sgrd", cached_prob, cached_values, preferred_element_type=jnp.float32
    )
    context = context + own_prob[..., None] * fresh_values[:, :, None, :]
    return context.reshape(seq_count, HEADS * HEAD_DIM).astype(jnp.bfloat16)


def dense_mixing(normed, router_weight, expert_ids):
    logits = jnp.dot(normed, router_weight, preferred_element_type=jnp.float32)
    expert_range = jnp.arange(router_weight.shape[1], dtype=jnp.int32)
    picked = jnp.any(expert_ids[:, :, None] == expert_range[None, None, :], axis=1)
    masked = jnp.where(picked, logits, -jnp.inf)
    raised = jnp.exp(masked - jnp.max(masked, axis=-1, keepdims=True))
    return raised / jnp.sum(raised, axis=-1, keepdims=True)


MESH = pl.DeviceIdType.MESH
AHEAD = 4
NEAR = 4


def greet(targets):
    barrier = pltpu.get_barrier_semaphore()

    expected = 0
    for condition, target in targets:
        signal = functools.partial(
            pl.semaphore_signal, barrier, inc=1, device_id=target, device_id_type=MESH
        )
        if condition is None:
            signal()
            expected = expected + 1
        else:
            pl.when(condition)(signal)
            expected = expected + condition.astype(jnp.int32)
    pl.semaphore_wait(barrier, expected)


def move_kernel(
    groups, count,
    gate_ref, up_ref, down_ref, rows_ref,
    gate_out, up_out, down_out, rows_out,
    send_w, recv_w, send_x, recv_x, local_sem, send_rows, recv_rows,
):
    me = lax.axis_index("expert")
    group = lax.axis_index("groups")
    parts = max(1, groups // 2)
    part_rows = gate_ref.shape[1] // parts
    part_columns = down_ref.shape[2] // groups
    line = count // 4
    layer = me // 4

    others = [(None, (group, me ^ r)) for r in range(1, count)]
    others += [(None, (lax.rem(group + h, groups), me)) for h in range(1, groups)]
    greet(others)

    def remote(src, dst, send, recv, target):
        return pltpu.make_async_remote_copy(
            src_ref=src, dst_ref=dst, send_sem=send, recv_sem=recv, device_id=target, device_id_type=MESH
        )

    def rows_of(owner):
        return pl.ds(pl.multiple_of((owner // 2) * part_rows, part_rows), part_rows)

    def columns_of(owner):
        return pl.ds(pl.multiple_of(owner * part_columns, part_columns), part_columns)

    def row_copy(kind, block, target, own=False):
        source = rows_ref if own else rows_out.at[block]
        return remote(
            source, rows_out.at[block], send_rows.at[kind, block], recv_rows.at[block], (group, target)
        )

    def row_wait(block):
        row_copy(0, block, me ^ 1).wait_recv()

    own_rows = pltpu.make_async_copy(rows_ref, rows_out.at[me], local_sem.at[3])
    own_rows.start()
    has_up, has_down = me + 4 < count, me >= 4

    @pl.when(has_up)
    def _():
        row_copy(0, me, me + 4, True).start()

    @pl.when(has_down)
    def _():
        row_copy(1, me, me - 4, True).start()

    row_copy(2, me, me ^ 2, True).start()
    row_copy(3, me, me ^ 1, True).start()

    def line_step(step):
        below, above = me - 4 * (step + 1), me + 4 * (step + 1)

        @pl.when(below >= 0)
        def _():
            row_wait(below)

            @pl.when(has_up)
            def _():
                row_copy(0, below, me + 4).start()

            row_copy(2, below, me ^ 2).start()
            row_copy(3, below, me ^ 1).start()

        @pl.when(above < count)
        def _():
            row_wait(above)

            @pl.when(has_down)
            def _():
                row_copy(1, above, me - 4).start()

            row_copy(2, above, me ^ 2).start()
            row_copy(3, above, me ^ 1).start()

    def side_step(index):
        block = lax.rem(me, 4) ^ 2
        block = block + 4 * index
        row_wait(block)
        row_copy(3, block, me ^ 1).start()

    def across(kind, r, refs_in, refs_out, which):
        target = me ^ r
        if r < NEAR:
            a, b = ((gate_ref, gate_out), (down_ref, down_out), (up_ref, up_out))[kind]
            send = send_x.at[0, r, 0] if kind == 2 else send_w.at[kind, r]
            recv = recv_x.at[0, r, 0] if kind == 2 else recv_w.at[kind, r]
            return remote(a.at[target], b.at[me], send, recv, (group, target))
        if kind == 0:
            return remote(
                refs_in[which].at[target, rows_of(group)], refs_out[which].at[me, rows_of(group)],
                send_w.at[0, r], recv_w.at[0, r], (group, target),
            )
        return remote(
            down_ref.at[target, :, columns_of(group)], down_out.at[me, :, columns_of(group)],
            send_w.at[1, r], recv_w.at[1, r], (group, target),
        )

    ins, outs = (gate_ref, up_ref), (gate_out, up_out)

    def by_matrix(act):
        pl.when(lax.rem(group, 2) == 0)(functools.partial(act, 0))
        pl.when(lax.rem(group, 2) == 1)(functools.partial(act, 1))

    def start_weight(kind, r):
        if kind == 0 and r >= NEAR:
            by_matrix(lambda which: across(0, r, ins, outs, which).start())
        else:
            across(kind, r, ins, outs, 0).start()

    def onward(kind, r, h, which):
        held = me ^ r
        place = outs[which].at[held, rows_of(group)] if kind == 0 else down_out.at[held, :, columns_of(group)]
        return remote(
            place, place, send_x.at[kind, r, h - 1], recv_x.at[kind, r, h - 1],
            (lax.rem(group + h, groups), me),
        )

    def pass_on(kind, r):
        across(kind, r, ins, outs, 0).wait_recv()
        for h in range(1, groups if r >= NEAR else 1):
            if kind == 0:
                by_matrix(lambda which: onward(0, r, h, which).start())
            else:
                onward(1, r, h, 0).start()

    own_copies = [
        pltpu.make_async_copy(a.at[me], b.at[me], local_sem.at[i])
        for i, (a, b) in enumerate(((gate_ref, gate_out), (up_ref, up_out), (down_ref, down_out)))
    ]
    half = count // 2
    order = [r for i in range(half) for r in ((half + i, i) if i else (half,))]
    first = [(kind, r) for r in order for kind in ((0, 2) if r < NEAR else (0,))]
    items = first + [(1, r) for r in order]
    spacing = len(items) // (line + 1)
    side_at = 2 + spacing * (line - 1) + 3
    for i, item in enumerate(items):
        start_weight(*item)
        if i >= 2 and (i - 2) % spacing == 0 and (i - 2) // spacing < line - 1:
            line_step((i - 2) // spacing)
        if i == side_at:
            for index in range(line):
                side_step(index)
        if i == AHEAD:
            for copy in own_copies:
                copy.start()
        if i >= AHEAD:
            pass_on(*items[i - AHEAD])
    for item in items[len(items) - AHEAD :]:
        pass_on(*item)

    for index in range(line):
        for y in range(2):
            row_wait(4 * index + 2 * y + (lax.rem(me, 2) ^ 1))
    own_rows.wait()
    for copy in own_copies:
        copy.wait()
    for kind, r in items:
        across(kind, r, ins, outs, 0).wait_send()
        for h in range(1, groups if r >= NEAR else 1):
            onward(kind, r, h, 0).wait()
    for index in range(line):
        block = lax.rem(me, 4) + 4 * index

        @pl.when(jnp.logical_and(has_up, index <= layer))
        def _():
            row_copy(0, block, me ^ 1).wait_send()

        @pl.when(jnp.logical_and(has_down, index >= layer))
        def _():
            row_copy(1, block, me ^ 1).wait_send()

        row_copy(2, block, me ^ 1).wait_send()
        row_copy(3, block, me ^ 1).wait_send()
        row_copy(3, block ^ 2, me ^ 1).wait_send()


def move(groups, gate_train, up_train, down_train, row_block):
    count = gate_train.shape[0]
    anywhere = pl.BlockSpec(memory_space=pl.ANY)
    DMA = pltpu.SemaphoreType.DMA
    return pl.pallas_call(
        functools.partial(move_kernel, groups, count),
        out_shape=[
            jax.ShapeDtypeStruct(gate_train.shape, gate_train.dtype),
            jax.ShapeDtypeStruct(up_train.shape, up_train.dtype),
            jax.ShapeDtypeStruct(down_train.shape, down_train.dtype),
            jax.ShapeDtypeStruct((count,) + row_block.shape, row_block.dtype),
        ],
        in_specs=[anywhere, anywhere, anywhere, pl.BlockSpec(memory_space=pltpu.VMEM)],
        out_specs=[anywhere] * 4,
        scratch_shapes=[
            DMA((2, count)), DMA((2, count)),
            DMA((2, count, max(1, groups - 1))), DMA((2, count, max(1, groups - 1))),
            DMA((4,)), DMA((4, count)), DMA((count,)),
        ],
        compiler_params=pltpu.CompilerParams(collective_id=0, has_side_effects=True),
    )(gate_train, up_train, down_train, row_block)


def sum_kernel(
    count, part_ref, out_ref, core_in, side_in, up_in, down_in, side_out, up_out, down_out,
    core_send, core_recv, side_send, side_recv, up_send, up_recv, down_send, down_recv,
):
    me = lax.axis_index("expert")
    group = lax.axis_index("groups")
    line, layer = count // 4, me // 4
    place = lax.rem(me, 4)
    side, core = place // 2, lax.rem(place, 2)
    has_up, has_down = me + 4 < count, me >= 4
    greet([
        (None, (group, me ^ 1)), (None, (group, me ^ 2)),
        (has_up, (group, me + 4)), (has_down, (group, me - 4)),
    ])
    chunk = 16
    row_count = part_ref.shape[1]

    def remote(src, dst, send, recv, target):
        return pltpu.make_async_remote_copy(
            src_ref=src, dst_ref=dst, send_sem=send, recv_sem=recv, device_id=(group, target), device_id_type=MESH
        )

    def add(target, *sources):
        @pl.loop(0, row_count // chunk)
        def _(step):
            rows = pl.ds(pl.multiple_of(step * chunk, chunk), chunk)
            total = sources[0][rows, :].astype(jnp.float32)
            for source in sources[1:]:
                total = total + source[rows, :].astype(jnp.float32)
            target[rows, :] = total.astype(target.dtype)

    def core_copy(at, y):
        slot = at * 2 + y
        return remote(
            part_ref.at[at * 4 + y * 2 + (core ^ 1)], core_in.at[slot], core_send.at[slot], core_recv.at[slot], me ^ 1
        )

    def side_copy(at):
        return remote(side_out.at[at], side_in.at[at], side_send.at[at], side_recv.at[at], me ^ 2)

    def up_copy(at):
        return remote(up_out.at[at], up_in.at[at], up_send.at[at], up_recv.at[at], me + 4)

    def down_copy(at):
        return remote(down_out.at[at], down_in.at[at], down_send.at[at], down_recv.at[at], me - 4)

    def in_order(act):
        for d in range(line - 1, 0, -1):
            pl.when(layer + d < line)(functools.partial(act, layer + d, 1))
            pl.when(layer - d >= 0)(functools.partial(act, layer - d, -1))
        act(layer, 0)

    in_order(lambda at, way: core_copy(at, side ^ 1).start())
    in_order(lambda at, way: core_copy(at, side).start())

    def to_side(at, way):
        core_copy(at, side ^ 1).wait_recv()
        add(side_out.at[at], part_ref.at[at * 4 + (side ^ 1) * 2 + core], core_in.at[at * 2 + (side ^ 1)])
        side_copy(at).start()

    in_order(to_side)

    def along(at, way):
        core_copy(at, side).wait_recv()
        side_copy(at).wait_recv()
        mine = (part_ref.at[at * 4 + place], core_in.at[at * 2 + side], side_in.at[at])
        if way == 1:
            @pl.when(has_down)
            def _():
                up_copy(at).wait_recv()
                add(up_out.at[at], *mine, up_in.at[at])

            @pl.when(jnp.logical_not(has_down))
            def _():
                add(up_out.at[at], *mine)

            up_copy(at).start()
        elif way == -1:
            @pl.when(has_up)
            def _():
                down_copy(at).wait_recv()
                add(down_out.at[at], *mine, down_in.at[at])

            @pl.when(jnp.logical_not(has_up))
            def _():
                add(down_out.at[at], *mine)

            down_copy(at).start()
        else:
            @pl.when(has_down)
            def _():
                up_copy(at).wait_recv()

            @pl.when(has_up)
            def _():
                down_copy(at).wait_recv()

            both = jnp.logical_and(has_down, has_up)

            @pl.when(both)
            def _():
                add(out_ref, *mine, up_in.at[at], down_in.at[at])

            @pl.when(jnp.logical_and(has_down, jnp.logical_not(has_up)))
            def _():
                add(out_ref, *mine, up_in.at[at])

            @pl.when(jnp.logical_and(has_up, jnp.logical_not(has_down)))
            def _():
                add(out_ref, *mine, down_in.at[at])

            @pl.when(jnp.logical_not(jnp.logical_or(has_up, has_down)))
            def _():
                add(out_ref, *mine)

    in_order(along)

    def finish(at, way):
        core_copy(at, side ^ 1).wait_send()
        core_copy(at, side).wait_send()
        side_copy(at).wait_send()
        if way == 1:
            up_copy(at).wait_send()
        if way == -1:
            down_copy(at).wait_send()

    in_order(finish)


def summed(partial_out, count):
    rows, width = partial_out.shape[0] // count, partial_out.shape[1]
    line = count // 4
    DMA = pltpu.SemaphoreType.DMA
    block = lambda amount: pltpu.VMEM((amount, rows, width), jnp.bfloat16)
    return pl.pallas_call(
        functools.partial(sum_kernel, count),
        out_shape=jax.ShapeDtypeStruct((rows, width), jnp.bfloat16),
        in_specs=[pl.BlockSpec(memory_space=pltpu.VMEM)],
        out_specs=pl.BlockSpec(memory_space=pltpu.VMEM),
        scratch_shapes=[block(count // 2)] + [block(line)] * 6
        + [DMA((count // 2,)), DMA((count // 2,))] + [DMA((line,))] * 6,
        compiler_params=pltpu.CompilerParams(collective_id=1, has_side_effects=True, vmem_limit_bytes=60 * 2**20),
    )(partial_out.reshape(count, rows, width))


def local(
    queries,
    key_cache,
    value_cache,
    new_key,
    new_value,
    cache_lengths,
    hidden_in,
    norm_gain,
    router_weight,
    expert_ids,
    gate_train,
    up_train,
    down_train,
):
    width = hidden_in.shape[1]
    expert_count = router_weight.shape[1]
    normed = rms_normed(hidden_in, norm_gain)
    mixing = dense_mixing(normed, router_weight, expert_ids)
    mixing_high = mixing.astype(jnp.bfloat16)
    mixing_low = (mixing - mixing_high.astype(jnp.float32)).astype(jnp.bfloat16)
    spare = -2 * expert_count % 128
    row_block = jnp.concatenate(
        [normed, mixing_high, mixing_low, jnp.zeros((normed.shape[0], spare), jnp.bfloat16)], axis=1
    )
    gate_moved, up_moved, down_moved, all_rows = move(
        lax.axis_size("groups"), gate_train, up_train, down_train, row_block
    )
    all_rows = all_rows.reshape(-1, all_rows.shape[-1])
    gate_moved = gate_moved.reshape(-1, gate_moved.shape[-1])
    up_moved = up_moved.reshape(-1, up_moved.shape[-1])
    down_moved = down_moved.reshape(-1, width)
    attended = attend(queries, key_cache, value_cache, new_key, new_value, cache_lengths)
    own_index = lax.axis_index("expert")
    tokens = all_rows[:, :width]
    mix_parts = all_rows[:, width : width + 2 * expert_count].astype(jnp.float32)
    own_column = jnp.arange(2 * expert_count) % expert_count == own_index
    own_mix = jnp.sum(jnp.where(own_column[None, :], mix_parts, 0.0), axis=1)
    gate_proj = jnp.dot(tokens, gate_moved, preferred_element_type=jnp.float32)
    up_proj = jnp.dot(tokens, up_moved, preferred_element_type=jnp.float32)
    hidden_units = (jax.nn.silu(gate_proj) * up_proj * own_mix[:, None]).astype(jnp.bfloat16)
    partial_out = jnp.dot(hidden_units, down_moved, preferred_element_type=jnp.float32).astype(jnp.bfloat16)
    mixed_out = summed(partial_out, expert_count)
    return (attended, mixed_out)


def solution(mesh):
    placed = (
        P(("groups", "expert"), None),
        P(("groups", "expert"), None, None),
        P(("groups", "expert"), None, None),
        P(("groups", "expert"), None),
        P(("groups", "expert"), None),
        P(("groups", "expert")),
        P(("groups", "expert"), None),
        P(),
        P(),
        P(("groups", "expert"), None),
        P(None, "expert", None),
        P(None, "expert", None),
        P(None, "expert", None),
    )
    return jax.shard_map(
        local,
        mesh=mesh,
        in_specs=placed,
        out_specs=(P(("groups", "expert"), None), P(("groups", "expert"), None)),
        check_vma=False,
    )
```

```python
import functools
import math

import jax
import jax.numpy as jnp
from jax import lax
from jax.experimental import pallas as pl
from jax.experimental.pallas import tpu as pltpu
from jax.sharding import PartitionSpec as P

HEADS = 32
KV_HEADS = 4
HEAD_DIM = 128
CTX = 64


EPSILON = 1e-06


def rms_normed(hidden_in, norm_gain):
    values = hidden_in.astype(jnp.float32)
    mean_square = jnp.mean(values * values, axis=-1, keepdims=True)
    return (values * lax.rsqrt(mean_square + EPSILON) * norm_gain.astype(jnp.float32)).astype(
        jnp.bfloat16
    )


def attend(queries, key_cache, value_cache, new_key, new_value, cache_lengths):
    seq_count = queries.shape[0]
    group_size = HEADS // KV_HEADS
    query_blocks = queries.reshape(seq_count, KV_HEADS, group_size, HEAD_DIM)
    cached_keys = key_cache.reshape(seq_count, CTX, KV_HEADS, HEAD_DIM)
    cached_values = value_cache.reshape(seq_count, CTX, KV_HEADS, HEAD_DIM)
    fresh_keys = new_key.reshape(seq_count, KV_HEADS, HEAD_DIM)
    fresh_values = new_value.astype(jnp.float32).reshape(seq_count, KV_HEADS, HEAD_DIM)
    score_scale = 1.0 / math.sqrt(HEAD_DIM)
    scores = (
        jnp.einsum("sgrd,scgd->sgrc", query_blocks, cached_keys, preferred_element_type=jnp.float32)
        * score_scale
    )
    own_score = (
        jnp.einsum("sgrd,sgd->sgr", query_blocks, fresh_keys, preferred_element_type=jnp.float32)
        * score_scale
    )
    positions = jnp.arange(CTX, dtype=jnp.int32)
    visible = positions[None, :] < cache_lengths[:, None]
    scores = jnp.where(visible[:, None, None, :], scores, -1e30)
    largest = jnp.maximum(jnp.max(scores, axis=-1), own_score)
    cached_exp = jnp.exp(scores - largest[..., None])
    own_exp = jnp.exp(own_score - largest)
    prob_total = jnp.sum(cached_exp, axis=-1) + own_exp
    cached_prob = (cached_exp / prob_total[..., None]).astype(jnp.bfloat16)
    own_prob = (own_exp / prob_total).astype(jnp.bfloat16).astype(jnp.float32)
    context = jnp.einsum(
        "sgrc,scgd->sgrd", cached_prob, cached_values, preferred_element_type=jnp.float32
    )
    context = context + own_prob[..., None] * fresh_values[:, :, None, :]
    return context.reshape(seq_count, HEADS * HEAD_DIM).astype(jnp.bfloat16)


def dense_mixing(normed, router_weight, expert_ids):
    logits = jnp.dot(normed, router_weight, preferred_element_type=jnp.float32)
    expert_range = jnp.arange(router_weight.shape[1], dtype=jnp.int32)
    picked = jnp.any(expert_ids[:, :, None] == expert_range[None, None, :], axis=1)
    masked = jnp.where(picked, logits, -jnp.inf)
    raised = jnp.exp(masked - jnp.max(masked, axis=-1, keepdims=True))
    return raised / jnp.sum(raised, axis=-1, keepdims=True)


MESH = pl.DeviceIdType.MESH
AHEAD = 4
NEAR = 4


def greet(targets):
    barrier = pltpu.get_barrier_semaphore()

    expected = 0
    for condition, target in targets:
        signal = functools.partial(
            pl.semaphore_signal, barrier, inc=1, device_id=target, device_id_type=MESH
        )
        if condition is None:
            signal()
            expected = expected + 1
        else:
            pl.when(condition)(signal)
            expected = expected + condition.astype(jnp.int32)
    pl.semaphore_wait(barrier, expected)


def move_kernel(
    groups, count,
    gate_ref, up_ref, down_ref, rows_ref,
    hidden_ref, down_out, gate_out, up_out, rows_out,
    send_w, recv_w, send_x, recv_x, local_sem, send_rows, recv_rows,
):
    me = lax.axis_index("expert")
    group = lax.axis_index("groups")
    parts = max(1, groups // 2)
    part_rows = gate_ref.shape[1] // parts
    part_columns = down_ref.shape[2] // groups
    line = count // 4
    layer = me // 4

    others = [(None, (group, me ^ r)) for r in range(1, count)]
    others += [(None, (lax.rem(group + h, groups), me)) for h in range(1, groups)]
    greet(others)

    def remote(src, dst, send, recv, target):
        return pltpu.make_async_remote_copy(
            src_ref=src, dst_ref=dst, send_sem=send, recv_sem=recv, device_id=target, device_id_type=MESH
        )

    def rows_of(owner):
        return pl.ds(pl.multiple_of((owner // 2) * part_rows, part_rows), part_rows)

    def columns_of(owner):
        return pl.ds(pl.multiple_of(owner * part_columns, part_columns), part_columns)

    def row_copy(kind, block, target, own=False):
        source = rows_ref if own else rows_out.at[block]
        return remote(
            source, rows_out.at[block], send_rows.at[kind, block], recv_rows.at[block], (group, target)
        )

    def row_wait(block):
        row_copy(0, block, me ^ 1).wait_recv()

    own_rows = pltpu.make_async_copy(rows_ref, rows_out.at[me], local_sem.at[3])
    own_rows.start()
    has_up, has_down = me + 4 < count, me >= 4

    @pl.when(has_up)
    def _():
        row_copy(0, me, me + 4, True).start()

    @pl.when(has_down)
    def _():
        row_copy(1, me, me - 4, True).start()

    row_copy(2, me, me ^ 2, True).start()
    row_copy(3, me, me ^ 1, True).start()

    def line_step(step):
        below, above = me - 4 * (step + 1), me + 4 * (step + 1)

        @pl.when(below >= 0)
        def _():
            row_wait(below)

            @pl.when(has_up)
            def _():
                row_copy(0, below, me + 4).start()

            row_copy(2, below, me ^ 2).start()
            row_copy(3, below, me ^ 1).start()

        @pl.when(above < count)
        def _():
            row_wait(above)

            @pl.when(has_down)
            def _():
                row_copy(1, above, me - 4).start()

            row_copy(2, above, me ^ 2).start()
            row_copy(3, above, me ^ 1).start()

    def side_step(index):
        block = lax.rem(me, 4) ^ 2
        block = block + 4 * index
        row_wait(block)
        row_copy(3, block, me ^ 1).start()

    def across(kind, r, refs_in, refs_out, which):
        target = me ^ r
        if r < NEAR:
            a, b = ((gate_ref, gate_out), (down_ref, down_out), (up_ref, up_out))[kind]
            send = send_x.at[0, r, 0] if kind == 2 else send_w.at[kind, r]
            recv = recv_x.at[0, r, 0] if kind == 2 else recv_w.at[kind, r]
            return remote(a.at[target], b.at[me], send, recv, (group, target))
        if kind == 0:
            return remote(
                refs_in[which].at[target, rows_of(group)], refs_out[which].at[me, rows_of(group)],
                send_w.at[0, r], recv_w.at[0, r], (group, target),
            )
        return remote(
            down_ref.at[target, :, columns_of(group)], down_out.at[me, :, columns_of(group)],
            send_w.at[1, r], recv_w.at[1, r], (group, target),
        )

    ins, outs = (gate_ref, up_ref), (gate_out, up_out)

    def by_matrix(act):
        pl.when(lax.rem(group, 2) == 0)(functools.partial(act, 0))
        pl.when(lax.rem(group, 2) == 1)(functools.partial(act, 1))

    def start_weight(kind, r):
        if kind == 0 and r >= NEAR:
            by_matrix(lambda which: across(0, r, ins, outs, which).start())
        else:
            across(kind, r, ins, outs, 0).start()

    def onward(kind, r, h, which):
        held = me ^ r
        place = outs[which].at[held, rows_of(group)] if kind == 0 else down_out.at[held, :, columns_of(group)]
        return remote(
            place, place, send_x.at[kind, r, h - 1], recv_x.at[kind, r, h - 1],
            (lax.rem(group + h, groups), me),
        )

    def pass_on(kind, r):
        across(kind, r, ins, outs, 0).wait_recv()
        for h in range(1, groups if r >= NEAR else 1):
            if kind == 0:
                by_matrix(lambda which: onward(0, r, h, which).start())
            else:
                onward(1, r, h, 0).start()

    own_copies = [
        pltpu.make_async_copy(a.at[me], b.at[me], local_sem.at[i])
        for i, (a, b) in enumerate(((gate_ref, gate_out), (up_ref, up_out), (down_ref, down_out)))
    ]
    width = gate_ref.shape[1] * count

    def ready():
        for index in range(line):
            for y in range(2):
                row_wait(4 * index + 2 * y + (lax.rem(me, 2) ^ 1))
        own_rows.wait()
        for copy in own_copies[:2]:
            copy.wait()
        for r in order:
            for h in range(1, groups if r >= NEAR else 1):
                onward(0, r, h, 0).wait_recv()

    def expert_rows(quarter):
        @pl.loop(0, count // 16)
        def _(step):
            at = quarter * (count // 4) + step * 4
            rows = rows_out[pl.ds(at, 4)].reshape(-1, rows_out.shape[2])
            tokens = rows[:, :width]
            shares = rows[:, width:].astype(jnp.float32)
            lane = lax.broadcasted_iota(jnp.int32, shares.shape, 1)
            own = jnp.logical_or(lane == me, lane == me + count)
            own_mix = jnp.sum(jnp.where(own, shares, 0.0), axis=1, keepdims=True)
            gate = gate_out[...].reshape(width, -1)
            gate_proj = jnp.dot(tokens, gate, preferred_element_type=jnp.float32)
            up = up_out[...].reshape(width, -1)
            up_proj = jnp.dot(tokens, up, preferred_element_type=jnp.float32)
            hidden = gate_proj / (1.0 + jnp.exp(-gate_proj)) * up_proj * own_mix
            place = pl.ds(pl.multiple_of(at * rows_out.shape[1], rows.shape[0]), rows.shape[0])
            hidden_ref[place, :] = hidden.astype(hidden_ref.dtype)

    half = count // 2
    order = [r for i in range(half) for r in ((half + i, i) if i else (half,))]
    first = [(kind, r) for r in order for kind in ((0, 2) if r < NEAR else (0,))]
    items = first + [(1, r) for r in order]
    spacing = len(items) // (line + 1)
    side_at = 2 + spacing * (line - 1) + 3

    def advance(i):
        pass_on(*items[i])
        before_last = len(items) - 1 - i
        if before_last % 2 == 0 and before_last < 8:
            if before_last == 6:
                ready()
            expert_rows(3 - before_last // 2)

    for i, item in enumerate(items):
        start_weight(*item)
        if i >= 2 and (i - 2) % spacing == 0 and (i - 2) // spacing < line - 1:
            line_step((i - 2) // spacing)
        if i == side_at:
            for index in range(line):
                side_step(index)
        if i == AHEAD:
            for copy in own_copies:
                copy.start()
        if i >= AHEAD:
            advance(i - AHEAD)
    for i in range(len(items) - AHEAD, len(items)):
        advance(i)

    own_copies[2].wait()
    for kind, r in items:
        across(kind, r, ins, outs, 0).wait_send()
        for h in range(1, groups if r >= NEAR else 1):
            onward(kind, r, h, 0).wait_send()
            if kind == 1:
                onward(kind, r, h, 0).wait_recv()
    for index in range(line):
        block = lax.rem(me, 4) + 4 * index

        @pl.when(jnp.logical_and(has_up, index <= layer))
        def _():
            row_copy(0, block, me ^ 1).wait_send()

        @pl.when(jnp.logical_and(has_down, index >= layer))
        def _():
            row_copy(1, block, me ^ 1).wait_send()

        row_copy(2, block, me ^ 1).wait_send()
        row_copy(3, block, me ^ 1).wait_send()
        row_copy(3, block ^ 2, me ^ 1).wait_send()


def move(groups, gate_train, up_train, down_train, row_block):
    count = gate_train.shape[0]
    anywhere = pl.BlockSpec(memory_space=pl.ANY)
    DMA = pltpu.SemaphoreType.DMA
    return pl.pallas_call(
        functools.partial(move_kernel, groups, count),
        out_shape=[
            jax.ShapeDtypeStruct((count * row_block.shape[0], gate_train.shape[2]), jnp.bfloat16),
            jax.ShapeDtypeStruct(down_train.shape, down_train.dtype),
        ],
        in_specs=[anywhere, anywhere, anywhere, pl.BlockSpec(memory_space=pltpu.VMEM)],
        out_specs=[pl.BlockSpec(memory_space=pltpu.VMEM), anywhere],
        scratch_shapes=[
            pltpu.VMEM(gate_train.shape, gate_train.dtype),
            pltpu.VMEM(up_train.shape, up_train.dtype),
            pltpu.VMEM((count,) + row_block.shape, row_block.dtype),
            DMA((2, count)), DMA((2, count)),
            DMA((2, count, max(1, groups - 1))), DMA((2, count, max(1, groups - 1))),
            DMA((4,)), DMA((4, count)), DMA((count,)),
        ],
        compiler_params=pltpu.CompilerParams(collective_id=0, has_side_effects=True, vmem_limit_bytes=60 * 2**20),
    )(gate_train, up_train, down_train, row_block)


def sum_kernel(
    count, part_ref, out_ref, core_in, side_in, up_in, down_in, side_out, up_out, down_out,
    core_send, core_recv, side_send, side_recv, up_send, up_recv, down_send, down_recv,
):
    me = lax.axis_index("expert")
    group = lax.axis_index("groups")
    line, layer = count // 4, me // 4
    place = lax.rem(me, 4)
    side, core = place // 2, lax.rem(place, 2)
    has_up, has_down = me + 4 < count, me >= 4
    greet([
        (None, (group, me ^ 1)), (None, (group, me ^ 2)),
        (has_up, (group, me + 4)), (has_down, (group, me - 4)),
    ])
    chunk = 16
    row_count = part_ref.shape[1]

    def remote(src, dst, send, recv, target):
        return pltpu.make_async_remote_copy(
            src_ref=src, dst_ref=dst, send_sem=send, recv_sem=recv, device_id=(group, target), device_id_type=MESH
        )

    def add(target, *sources):
        @pl.loop(0, row_count // chunk)
        def _(step):
            rows = pl.ds(pl.multiple_of(step * chunk, chunk), chunk)
            total = sources[0][rows, :].astype(jnp.float32)
            for source in sources[1:]:
                total = total + source[rows, :].astype(jnp.float32)
            target[rows, :] = total.astype(target.dtype)

    def core_copy(at, y):
        slot = at * 2 + y
        return remote(
            part_ref.at[at * 4 + y * 2 + (core ^ 1)], core_in.at[slot], core_send.at[slot], core_recv.at[slot], me ^ 1
        )

    def side_copy(at):
        return remote(side_out.at[at], side_in.at[at], side_send.at[at], side_recv.at[at], me ^ 2)

    def up_copy(at):
        return remote(up_out.at[at], up_in.at[at], up_send.at[at], up_recv.at[at], me + 4)

    def down_copy(at):
        return remote(down_out.at[at], down_in.at[at], down_send.at[at], down_recv.at[at], me - 4)

    def in_order(act):
        for d in range(line - 1, 0, -1):
            pl.when(layer + d < line)(functools.partial(act, layer + d, 1))
            pl.when(layer - d >= 0)(functools.partial(act, layer - d, -1))
        act(layer, 0)

    in_order(lambda at, way: core_copy(at, side ^ 1).start())
    in_order(lambda at, way: core_copy(at, side).start())

    def to_side(at, way):
        core_copy(at, side ^ 1).wait_recv()
        add(side_out.at[at], part_ref.at[at * 4 + (side ^ 1) * 2 + core], core_in.at[at * 2 + (side ^ 1)])
        side_copy(at).start()

    in_order(to_side)

    def along(at, way):
        core_copy(at, side).wait_recv()
        side_copy(at).wait_recv()
        mine = (part_ref.at[at * 4 + place], core_in.at[at * 2 + side], side_in.at[at])
        if way == 1:
            @pl.when(has_down)
            def _():
                up_copy(at).wait_recv()
                add(up_out.at[at], *mine, up_in.at[at])

            @pl.when(jnp.logical_not(has_down))
            def _():
                add(up_out.at[at], *mine)

            up_copy(at).start()
        elif way == -1:
            @pl.when(has_up)
            def _():
                down_copy(at).wait_recv()
                add(down_out.at[at], *mine, down_in.at[at])

            @pl.when(jnp.logical_not(has_up))
            def _():
                add(down_out.at[at], *mine)

            down_copy(at).start()
        else:
            @pl.when(has_down)
            def _():
                up_copy(at).wait_recv()

            @pl.when(has_up)
            def _():
                down_copy(at).wait_recv()

            both = jnp.logical_and(has_down, has_up)

            @pl.when(both)
            def _():
                add(out_ref, *mine, up_in.at[at], down_in.at[at])

            @pl.when(jnp.logical_and(has_down, jnp.logical_not(has_up)))
            def _():
                add(out_ref, *mine, up_in.at[at])

            @pl.when(jnp.logical_and(has_up, jnp.logical_not(has_down)))
            def _():
                add(out_ref, *mine, down_in.at[at])

            @pl.when(jnp.logical_not(jnp.logical_or(has_up, has_down)))
            def _():
                add(out_ref, *mine)

    in_order(along)

    def finish(at, way):
        core_copy(at, side ^ 1).wait_send()
        core_copy(at, side).wait_send()
        side_copy(at).wait_send()
        if way == 1:
            up_copy(at).wait_send()
        if way == -1:
            down_copy(at).wait_send()

    in_order(finish)


def summed(partial_out, count):
    rows, width = partial_out.shape[0] // count, partial_out.shape[1]
    line = count // 4
    DMA = pltpu.SemaphoreType.DMA
    block = lambda amount: pltpu.VMEM((amount, rows, width), jnp.bfloat16)
    return pl.pallas_call(
        functools.partial(sum_kernel, count),
        out_shape=jax.ShapeDtypeStruct((rows, width), jnp.bfloat16),
        in_specs=[pl.BlockSpec(memory_space=pltpu.VMEM)],
        out_specs=pl.BlockSpec(memory_space=pltpu.VMEM),
        scratch_shapes=[block(count // 2)] + [block(line)] * 6
        + [DMA((count // 2,)), DMA((count // 2,))] + [DMA((line,))] * 6,
        compiler_params=pltpu.CompilerParams(collective_id=1, has_side_effects=True, vmem_limit_bytes=60 * 2**20),
    )(partial_out.reshape(count, rows, width))


def local(
    queries,
    key_cache,
    value_cache,
    new_key,
    new_value,
    cache_lengths,
    hidden_in,
    norm_gain,
    router_weight,
    expert_ids,
    gate_train,
    up_train,
    down_train,
):
    width = hidden_in.shape[1]
    expert_count = router_weight.shape[1]
    normed = rms_normed(hidden_in, norm_gain)
    mixing = dense_mixing(normed, router_weight, expert_ids)
    mixing_high = mixing.astype(jnp.bfloat16)
    mixing_low = (mixing - mixing_high.astype(jnp.float32)).astype(jnp.bfloat16)
    spare = -2 * expert_count % 128
    row_block = jnp.concatenate(
        [normed, mixing_high, mixing_low, jnp.zeros((normed.shape[0], spare), jnp.bfloat16)], axis=1
    )
    hidden_units, down_moved = move(
        lax.axis_size("groups"), gate_train, up_train, down_train, row_block
    )
    down_moved = down_moved.reshape(-1, width)
    attended = attend(queries, key_cache, value_cache, new_key, new_value, cache_lengths)
    partial_out = jnp.dot(hidden_units, down_moved, preferred_element_type=jnp.float32).astype(jnp.bfloat16)
    mixed_out = summed(partial_out, expert_count)
    return (attended, mixed_out)


def solution(mesh):
    placed = (
        P(("groups", "expert"), None),
        P(("groups", "expert"), None, None),
        P(("groups", "expert"), None, None),
        P(("groups", "expert"), None),
        P(("groups", "expert"), None),
        P(("groups", "expert")),
        P(("groups", "expert"), None),
        P(),
        P(),
        P(("groups", "expert"), None),
        P(None, "expert", None),
        P(None, "expert", None),
        P(None, "expert", None),
    )
    return jax.shard_map(
        local,
        mesh=mesh,
        in_specs=placed,
        out_specs=(P(("groups", "expert"), None), P(("groups", "expert"), None)),
        check_vma=False,
    )
```
